128 devices in a mesh: gx: 4 (over y_hi, core), gy: 4 (over z), gz: 8 (over y_lo, x).
Axes of the slice: x: 4, y: 4 (y_hi: 2, y_lo: 2; y = y_hi * 2 + y_lo), z: 4, core: 2. Of those that a mesh axis runs over, the one named last changes fastest.
Arguments:
- inputs: bfloat16 [131072, 2048], P(('gx', 'gy', 'gz')), may hold values from -24 to 24
- cotangent: bfloat16 [131072, 4096], P(('gx', 'gy', 'gz')), may hold values from -0.016479492 to 0.016479492
- master: float32 [2048, 4096], P(('gx', 'gy', 'gz')), may hold values from -3 to 3
- accum: float32 [2048, 4096], P(('gx', 'gy', 'gz')), may hold values from 0.05 to 1
Outputs:
- new_master: float32 [2048, 4096], P(('gx', 'gy', 'gz'))
- new_accum: float32 [2048, 4096], P(('gx', 'gy', 'gz'))
The draws below stay inside these ranges and needn't reach their ends.
All inputs are finite; a program needn't handle non-finite values.
Results may differ from the reference program's by a relative error of at most 0.0003.
Values sent between devices are 32-bit elements; how exact they have to be, the bound alone decides.
No kernel may reach another device: no remote copies, remote signals or barrier semaphores. Data moves between devices by JAX's collectives and lax.ppermute only.
A program may use at most 128 MiB of HBM per device.

```python
import math
import jax
import jax.numpy as jnp
from jax import lax

D = 4096
ROWS = 2048
TOKENS = 131072


def spiked(drawn, rng, source, target, shards_of, factor):
    owner, partner = [(jnp.arange(drawn.shape[position]) // (drawn.shape[position] // shards_of)).reshape([-1 if axis == position else 1 for axis in range(drawn.ndim)]) for position in (source, target)]
    chosen = jax.random.permutation(rng, shards_of)[partner]
    strong = (owner == chosen) | (owner == (partner + shards_of // 2) % shards_of)
    return jnp.where(strong, factor * drawn, drawn)


def shard_levels(rng, shape, shards, low, high):
    factor_of, own = 1.0, jax.random.fold_in(rng, 6)
    for axis_at, parts in shards:
        steps = jnp.exp(jax.random.uniform(jax.random.fold_in(own, axis_at), (parts,), jnp.float32, low / len(shards), high / len(shards)))
        factor_of = factor_of * jnp.repeat(steps, shape[axis_at] // parts).reshape([-1 if axis == axis_at else 1 for axis in range(len(shape))])
    return factor_of


def bell_draw(stream_key, dims, spread, most, cuts=(), dtype=jnp.bfloat16):
    array = spread * jax.random.normal(stream_key, dims, jnp.float32)
    if cuts:
        array = array * shard_levels(stream_key, dims, cuts, -0.22, 0.18)
    return jnp.clip(array, -most, most).astype(dtype)


def heavy_noise(own_key, dims, width, most, split, heavy, dtype=jnp.bfloat16):
    values = width * jax.random.normal(own_key, dims, jnp.float32)
    if split:
        values = values * shard_levels(own_key, dims, split, -0.22, 0.18)
    return jnp.clip(spiked(values, jax.random.fold_in(own_key, 3), *heavy), -most, most).astype(dtype)


def setup_inputs(seed: int = 0) -> dict:
    key_list = jax.random.split(jax.random.key(seed), 5)
    return {
        "inputs": heavy_noise(key_list[0], (TOKENS, ROWS), 1.0, 24.0, ((0, 128),), (0, 1, 128, 5.5)),
        "cotangent": bell_draw(key_list[1], (TOKENS, D), (TOKENS ** -0.5), 0.016479492, ((0, 128),)),
        "master": bell_draw(key_list[2], (ROWS, D), 0.5, 3.0, ((0, 128),), jnp.float32),
        "accum": jnp.clip(jnp.exp(math.log(1.0) - 2.9957323 * jax.random.uniform(key_list[3], (ROWS, D), jnp.float32) ** shard_levels(key_list[3], (ROWS, D), ((0, 128),), -0.2, 0.2)), 0.05, 1.0),
    }


def reference(inputs, cotangent, master, accum):
    gradient = lax.dot_general(inputs, cotangent, (((0,), (0,)), ((), ())), preferred_element_type=jnp.float32)
    squares = jnp.sum(gradient * gradient)
    limit = 0.5 * jnp.sqrt(jnp.float32(ROWS * D))
    factor = limit / jnp.maximum(jnp.sqrt(squares), limit)
    scaled = factor * gradient
    new_accum = accum + scaled * scaled
    new_master = master - 0.5 * scaled / jnp.sqrt(new_accum)
    return (new_master, new_accum)
```

```python
import functools

import jax
import jax.numpy as jnp
from jax import lax
from jax.experimental import pallas as pl
from jax.experimental.pallas import tpu as pltpu
from jax.sharding import Mesh
from jax.sharding import PartitionSpec as P

D = 4096
ROWS = 2048
TOK = 1024
BLK = 16
F32 = jnp.float32
ALL = ("gx_0", "gx_1", "gy", "gz_0", "gz_1")
DEVICES = 128


CORE = 32
XA, XB, YA, YB, ZA, ZB = 1, 3, 4, 68, 8, 24
GROUPS = ((XA, YA, ZA), (XB, YB, ZB))
WIDTHS = (768, 768, 640, 640, 640, 640)
OFFSETS = tuple(sum(WIDTHS[:i]) for i in range(6))


def color_dims(color):
    group, turn = divmod(color, 3)
    first = GROUPS[group]
    return tuple(first[(turn + s) % 3] for s in range(3)), GROUPS[1 - group]


def span(masks):
    offsets = [0]
    for mask in reversed(masks):
        offsets = offsets + [mask ^ o for o in offsets]
    return offsets


def rows_of(color, send):
    first, rest = color_dims(color)
    return [(first[0] if send else 0) ^ o for o in span(first[1:] + rest)]


def hop(array, mask):
    return lax.ppermute(array, ALL, [(i, i ^ mask) for i in range(DEVICES)])


def transpose_body(x_ref, out_ref):
    out_ref[...] = x_ref[...].T


def transposed(inputs):
    return pl.pallas_call(
        transpose_body,
        grid=(ROWS // 256,),
        in_specs=[pl.BlockSpec((TOK, 256), lambda i: (0, i))],
        out_specs=pl.BlockSpec((256, TOK), lambda i: (i, 0)),
        out_shape=jax.ShapeDtypeStruct((ROWS, TOK), jnp.bfloat16),
        name="turn",
        cost_estimate=pl.CostEstimate(
            flops=2 * ROWS * TOK, bytes_accessed=4 * ROWS * TOK, transcendentals=0
        ),
    )(inputs)


def product_body(colors, send, flip, joined, added, me_ref, x_ref, c_ref, *refs):
    lhs = refs[-1]
    extra = refs[0] if added else None
    outs = refs[1:-1] if added else refs[:-1]
    me = me_ref[0]
    for n, color in enumerate(colors):
        for k, offset in enumerate(rows_of(color, send)):
            block = (me ^ (offset ^ flip)) * BLK
            lhs[k * BLK : (k + 1) * BLK, :] = x_ref[
                pl.ds(pl.multiple_of(block, BLK), BLK), :
            ]
        start, width = OFFSETS[color], WIDTHS[color]
        for at in range(0, width, 256):
            size = min(256, width - at)
            value = jnp.dot(
                lhs[...],
                c_ref[:, start + at : start + at + size],
                preferred_element_type=F32,
            )
            if joined:
                where = slice(start + at, start + at + size)
                if added:
                    value = value + extra[:, where]
                outs[0][:, where] = value
            else:
                outs[n][:, at : at + size] = value


def product(me, turned, cotangent, colors, send, flip, extra=None, joined=False):
    added = extra is not None
    rows = ROWS // 4
    if joined:
        shapes = [(rows, D)]
    else:
        shapes = [(rows, WIDTHS[c]) for c in colors]
    columns = sum(WIDTHS[c] for c in colors)
    vmem = pl.BlockSpec(memory_space=pltpu.VMEM)
    operands = (me, turned, cotangent) + ((extra,) if added else ())
    return pl.pallas_call(
        functools.partial(product_body, colors, send, flip, joined, added),
        in_specs=[pl.BlockSpec(memory_space=pltpu.SMEM)] + [vmem] * (len(operands) - 1),
        out_specs=[vmem] * len(shapes),
        out_shape=[jax.ShapeDtypeStruct(s, F32) for s in shapes],
        scratch_shapes=[pltpu.VMEM((rows, TOK), jnp.bfloat16)],
        compiler_params=pltpu.CompilerParams(vmem_limit_bytes=60 * 2**20),
        name="product",
        cost_estimate=pl.CostEstimate(
            flops=2 * rows * TOK * columns,
            bytes_accessed=4 * rows * columns,
            transcendentals=0,
        ),
    )(*operands)


def shards(inputs, cotangent, master, accum):
    me = lax.axis_index(ALL)
    at = me.astype(jnp.int32)[None]
    turned = transposed(inputs)
    every = tuple(range(6))
    theirs = product(at, turned, cotangent, every, True, CORE)
    theirs = [hop(t, CORE) for t in theirs]
    ours = product(at, turned, cotangent, every, True, 0)
    first = [hop(o + t, color_dims(c)[0][0]) for c, (o, t) in enumerate(zip(ours, theirs))]
    (kept_theirs,) = product(at, turned, cotangent, every, False, CORE, joined=True)
    kept_theirs = hop(kept_theirs, CORE)
    (kept,) = product(at, turned, cotangent, every, False, 0, kept_theirs, joined=True)

    finals = []
    for c in every:
        dims = color_dims(c)[0]
        cols = slice(OFFSETS[c], OFFSETS[c] + WIDTHS[c])
        second = hop(kept[256:, cols] + first[c][256:], dims[1])
        third = hop(
            kept[128:256, cols] + first[c][128:256] + second[128:], dims[2]
        )
        finals.append(
            kept[:128, cols] + first[c][:128] + second[:128] + third
        )

    halves = []
    for g in range(2):
        masks = span(GROUPS[1 - g])
        parts = finals[3 * g : 3 * g + 3]
        blocks = [
            jnp.concatenate([p[q * BLK : (q + 1) * BLK] for p in parts], axis=1)
            for q in range(8)
        ]
        total = blocks[0]
        for q in (7, 6, 5, 3, 4, 2, 1):
            total = total + hop(blocks[q], masks[q])
        halves.append(total)
    gradient = jnp.concatenate(halves, axis=1)

    local = jnp.sum(gradient * gradient)
    spread = jnp.broadcast_to(local, (DEVICES, 1, 128))
    squares = jnp.sum(lax.all_to_all(spread, ALL, 0, 0, tiled=True)[:, 0, 0])
    limit = 0.5 * jnp.sqrt(jnp.float32(ROWS * D))
    factor = limit / jnp.maximum(jnp.sqrt(squares), limit)
    scaled = factor * gradient
    new_accum = accum + scaled * scaled
    new_master = master - 0.5 * scaled / jnp.sqrt(new_accum)
    return (new_master, new_accum)


def solution(mesh):
    finer = Mesh(
        mesh.devices.reshape(2, 2, mesh.shape["gy"], 2, 4),
        ("gx_0", "gx_1", "gy", "gz_0", "gz_1"),
    )
    placed = P(ALL, None)
    return jax.shard_map(
        shards,
        mesh=finer,
        in_specs=(placed,) * 4,
        out_specs=(placed,) * 2,
        check_vma=False,
    )
```
